32 devices in a mesh: dp: 1 (over z), ep2: 4 (over y), ep: 8 (over x, core).
Axes of the slice: x: 4, y: 4, z: 1, core: 2. Of those that a mesh axis runs over, the one named last changes fastest.
The devices are a block of a 4x4x8 slice.
Arguments:
- tokens: bfloat16 [4096, 2048], P(('dp', 'ep2', 'ep'))
- expert_idx: int32 [4096, 4], P(('dp', 'ep2', 'ep'))
- gates: float32 [4096, 4], P(('dp', 'ep2', 'ep'))
- w_gate: bfloat16 [32, 2048, 1792], P(('ep2', 'ep'))
- w_up: bfloat16 [32, 2048, 1792], P(('ep2', 'ep'))
- w_down: bfloat16 [32, 1792, 2048], P(('ep2', 'ep'))
Outputs:
- output: bfloat16 [4096, 2048], P(('dp', 'ep2', 'ep'))
All inputs are finite; a program needn't handle non-finite values.
Results may differ from the reference program's by a relative error of at most 0.00107.
Values are sent between devices in bfloat16 or wider.
A program may use at most 768 MiB of HBM per device.

```python
import jax
import jax.numpy as jnp
from jax import lax

GROUP_DEVS = 32
TOKENS = 128
HIDDEN = 2048
EXPERT_FF = 1792
EXPERTS = 32
TOP_K = 4

LOCAL_EXPERTS = EXPERTS // GROUP_DEVS
EXPERT_CAP = (TOKENS * TOP_K + EXPERTS - 1) // EXPERTS
TOTAL_ROWS = GROUP_DEVS * TOKENS
EXPERT_ROWS = GROUP_DEVS * EXPERT_CAP


def draw_routing(route_key):
    key_pick, key_first, key_rest, key_bias = jax.random.split(route_key, 4)
    expert_ids = jnp.arange(EXPERTS, dtype=jnp.int32)
    local_pick = jax.random.randint(key_pick, (GROUP_DEVS, GROUP_DEVS), 0, LOCAL_EXPERTS)
    picked = (expert_ids % LOCAL_EXPERTS)[None, :] == jnp.repeat(local_pick, LOCAL_EXPERTS, axis=1)
    first_score = jax.random.randint(key_first, (GROUP_DEVS, EXPERTS), 0, 1024) + 2048
    rest_score = jax.random.randint(key_rest, (GROUP_DEVS, EXPERTS), 0, 1024) + jax.random.randint(key_bias, (1, EXPERTS), 0, 512)
    score = jnp.where(picked, first_score, rest_score) * EXPERTS + expert_ids[None, :]
    sequence = jnp.argsort(-score, axis=1).astype(jnp.int32)
    positions = (jnp.arange(TOKENS)[:, None] * TOP_K + jnp.arange(TOP_K)[None, :]) % EXPERTS
    chosen = jnp.take(sequence, positions.reshape(-1), axis=1)
    return chosen.reshape(TOTAL_ROWS, TOP_K)


def setup_inputs(seed: int = 0, part: int = 0) -> dict:
    root_key = jax.random.key(seed)
    shared_key, local_root = jax.random.split(root_key)
    part_key = jax.random.fold_in(local_root, part)
    key_tok, key_route, key_gate = jax.random.split(part_key, 3)
    key_wg, key_wu, key_wd = jax.random.split(shared_key, 3)
    tokens = jax.random.normal(key_tok, (TOTAL_ROWS, HIDDEN), jnp.float32).astype(jnp.bfloat16)
    expert_idx = draw_routing(key_route)
    gate_logits = jax.random.normal(key_gate, (TOTAL_ROWS, TOP_K), jnp.float32)
    gates = 0.5 * TOP_K * jax.nn.softmax(gate_logits, axis=-1)
    w_gate = (jax.random.normal(key_wg, (EXPERTS, HIDDEN, EXPERT_FF), jnp.float32) * HIDDEN ** -0.5).astype(jnp.bfloat16)
    w_up = (jax.random.normal(key_wu, (EXPERTS, HIDDEN, EXPERT_FF), jnp.float32) * HIDDEN ** -0.5).astype(jnp.bfloat16)
    w_down = (jax.random.normal(key_wd, (EXPERTS, EXPERT_FF, HIDDEN), jnp.float32) * EXPERT_FF ** -0.5).astype(jnp.bfloat16)
    return {'tokens': tokens, 'expert_idx': expert_idx, 'gates': gates, 'w_gate': w_gate, 'w_up': w_up, 'w_down': w_down}


def expert_ffn(operands):
    rows_in, gate_w, up_w, down_w = operands
    act_gate = jnp.dot(rows_in, gate_w, preferred_element_type=jnp.float32)
    act_up = jnp.dot(rows_in, up_w, preferred_element_type=jnp.float32)
    inner_act = (jax.nn.silu(act_gate) * act_up).astype(jnp.bfloat16)
    return jnp.dot(inner_act, down_w, preferred_element_type=jnp.float32).astype(jnp.bfloat16)


def reference(tokens, expert_idx, gates, w_gate, w_up, w_down):
    flat_ids = expert_idx.reshape(-1)
    n_items = flat_ids.shape[0]
    sort_order = jnp.argsort(flat_ids, stable=True)
    sorted_ids = flat_ids[sort_order]
    counts = jnp.bincount(flat_ids, length=EXPERTS)
    starts = jnp.cumsum(counts) - counts
    rank_sorted = (jnp.arange(n_items) - starts[sorted_ids]).astype(jnp.int32)
    slot_rank = jnp.zeros((n_items,), jnp.int32).at[sort_order].set(rank_sorted)
    token_of = jnp.arange(n_items) // TOP_K
    expert_in = jnp.zeros((EXPERTS, EXPERT_ROWS, HIDDEN), tokens.dtype).at[flat_ids, slot_rank].set(tokens[token_of])
    expert_out = lax.map(expert_ffn, (expert_in, w_gate, w_up, w_down))
    routed = expert_out[flat_ids, slot_rank].reshape(TOTAL_ROWS, TOP_K, HIDDEN)
    mixed = jnp.sum(gates[:, :, None] * routed.astype(jnp.float32), axis=1)
    return (tokens.astype(jnp.float32) + mixed).astype(jnp.bfloat16)
```

```python
import functools

import jax
import jax.numpy as jnp
from jax import lax
from jax.experimental import pallas as pl
from jax.experimental.pallas import tpu as pltpu
from jax.sharding import PartitionSpec as P

MESH = pl.DeviceIdType.MESH
BF16, F32, I32 = jnp.bfloat16, jnp.float32, jnp.int32
N_GROUPS = 4


def offsets_in_order(n_outer, n_inner):
    chips = n_inner // 2
    all_offsets = [(dy, dx, dc) for dc in (0, 1) for dy in range(n_outer) for dx in range(chips)]

    def hops(o):
        dy, dx, dc = o
        return min(dy, n_outer - dy) + min(dx, chips - dx)

    own = (0, 0, 0)
    far = sorted((o for o in all_offsets if o != own), key=lambda o: -hops(o))
    return [own] + far


def layer_kernel(order, n_outer, n_inner, idx_hbm, gate_hbm, tok_hbm, wg_hbm, wu_hbm, wd_hbm, out_ref,
                 idx_ref, gts_ref, tok_ref, wg_ref, wu_ref, wd_ref, slot_ref, sel_ref, perm_ref, gcol_ref,
                 send_ref, recv_ref, h_ref, y_ref, ret_ref,
                 in_sem, w_sem, out_send, out_recv, back_send, back_recv):
    dp, outer, inner = lax.axis_index('dp'), lax.axis_index('ep2'), lax.axis_index('ep')
    chips = n_inner // 2
    chip, core = inner // 2, inner % 2
    n_dev = n_outer * n_inner
    rows, d_model = tok_ref.shape
    top_k = idx_ref.shape[0]
    cap = (rows * top_k) // n_dev
    d_ff = wg_ref.shape[1]
    n_slots = n_dev * cap
    per_group = n_dev // N_GROUPS
    g_rows = n_slots // N_GROUPS

    def peer(o, sign):
        dy, dx, dc = o
        y = lax.rem(outer + (dy if sign > 0 else n_outer - dy), n_outer)
        x = lax.rem(chip + (dx if sign > 0 else chips - dx), chips)
        c = lax.rem(core + dc, 2)
        return y, x * 2 + c

    barrier = pltpu.get_barrier_semaphore()
    for o in order[1:]:
        y, x = peer(o, 1)
        pl.semaphore_signal(barrier, inc=1, device_id=(dp, y, x), device_id_type=MESH)

    idx_copy = pltpu.make_async_copy(idx_hbm, idx_ref, in_sem.at[0])
    tok_copy = pltpu.make_async_copy(tok_hbm, tok_ref, in_sem.at[1])
    gts_copy = pltpu.make_async_copy(gate_hbm, gts_ref, in_sem.at[2])
    w_copies = [pltpu.make_async_copy(h.at[0], v, w_sem.at[i])
                for i, (h, v) in enumerate(((wg_hbm, wg_ref), (wu_hbm, wu_ref), (wd_hbm, wd_ref)))]
    for copy in (idx_copy, tok_copy, gts_copy, *w_copies):
        copy.start()

    idx_copy.wait()
    expert = lax.broadcasted_iota(I32, (n_dev, rows), 0)
    chosen = jnp.zeros((n_dev, rows), F32)
    for j in range(top_k):
        chosen = chosen + jnp.where(idx_ref[j:j + 1, :] == expert, 1.0, 0.0)
    earlier = lax.broadcasted_iota(I32, (rows, rows), 0) < lax.broadcasted_iota(I32, (rows, rows), 1)
    rank = jnp.dot(chosen.astype(BF16), jnp.where(earlier, 1.0, 0.0).astype(BF16), preferred_element_type=F32)
    slot_ref[...] = jnp.where(chosen > 0.5, rank, -1.0)
    place = lax.broadcasted_iota(I32, (cap, rows), 0).astype(F32)
    for q, o in enumerate(order):
        y, x = peer(o, 1)
        row = slot_ref[pl.ds(y * n_inner + x, 1), :]
        sel_ref[q * cap:(q + 1) * cap, :] = jnp.where(row == place, 1.0, 0.0).astype(BF16)

    tok_copy.wait()
    for g in range(N_GROUPS):
        block = sel_ref[g * g_rows:(g + 1) * g_rows, :]
        send_ref[g * g_rows:(g + 1) * g_rows, :] = jnp.dot(block, tok_ref[...], preferred_element_type=F32).astype(BF16)
    pl.semaphore_wait(barrier, n_dev - 1)

    def copy_out(q):
        y, x = peer(order[q], 1)
        part = pl.ds(q * cap, cap)
        return pltpu.make_async_remote_copy(send_ref.at[part], recv_ref.at[part], out_send.at[q], out_recv.at[q],
                                            device_id=(dp, y, x), device_id_type=MESH)

    def copy_back(q):
        y, x = peer(order[q], -1)
        part = pl.ds(q * cap, cap)
        return pltpu.make_async_remote_copy(y_ref.at[part], ret_ref.at[part], back_send.at[q], back_recv.at[q],
                                            device_id=(dp, y, x), device_id_type=MESH)

    for q in range(1, n_dev):
        copy_out(q).start()
    recv_ref[0:cap, :] = send_ref[0:cap, :]

    gts_copy.wait()
    gcol_ref[...] = jnp.transpose(jnp.concatenate([gts_ref[...], jnp.zeros((8 - top_k, rows), F32)], axis=0))
    for g in range(N_GROUPS):
        for j in range(top_k):
            parts = []
            for q in range(g * per_group, (g + 1) * per_group):
                y, x = peer(order[q], 1)
                mine = jnp.where(idx_ref[j:j + 1, :] == y * n_inner + x, 1.0, 0.0)
                parts.append(sel_ref[q * cap:(q + 1) * cap, :].astype(F32) * mine)
            perm_ref[j * rows:(j + 1) * rows, g * g_rows:(g + 1) * g_rows] = jnp.transpose(
                jnp.concatenate(parts, axis=0)).astype(BF16)

    for g in range(N_GROUPS):
        for q in range(g * per_group, (g + 1) * per_group):
            if q:
                copy_out(q).wait_recv()
        part = pl.ds(g * g_rows, g_rows)
        if g == 0:
            w_copies[0].wait()
            w_copies[1].wait()

        def up(n, _):
            cols = pl.ds(pl.multiple_of(n * 256, 256), 256)
            a = jnp.dot(recv_ref[part, :], wg_ref[:, cols], preferred_element_type=F32)
            b = jnp.dot(recv_ref[part, :], wu_ref[:, cols], preferred_element_type=F32)
            h_ref[:, cols] = (jax.nn.silu(a) * b).astype(BF16)
            return 0

        lax.fori_loop(0, d_ff // 256, up, 0)
        if g == 0:
            w_copies[2].wait()

        def down(n, _):
            cols = pl.ds(pl.multiple_of(n * 256, 256), 256)
            y_ref[part, cols] = jnp.dot(h_ref[...], wd_ref[:, cols], preferred_element_type=F32).astype(BF16)
            return 0

        lax.fori_loop(0, d_model // 256, down, 0)
        for q in range(g * per_group, (g + 1) * per_group):
            if q:
                copy_back(q).start()
    ret_ref[0:cap, :] = y_ref[0:cap, :]

    for g in range(N_GROUPS):
        for q in range(g * per_group, (g + 1) * per_group):
            if q:
                copy_back(q).wait_recv()

        def combine(n, _):
            cols = pl.ds(pl.multiple_of(n * 256, 256), 256)
            routed = jnp.dot(perm_ref[:, g * g_rows:(g + 1) * g_rows], ret_ref[g * g_rows:(g + 1) * g_rows, cols],
                             preferred_element_type=F32)
            total = gcol_ref[:, 0:1] * routed[0:rows]
            for j in range(1, top_k):
                total = total + gcol_ref[:, j:j + 1] * routed[j * rows:(j + 1) * rows]
            out_ref[:, cols] = total if g == 0 else out_ref[:, cols] + total
            return 0

        lax.fori_loop(0, d_model // 256, combine, 0)
    for q in range(1, n_dev):
        copy_out(q).wait_send()
        copy_back(q).wait_send()


def solution(mesh):
    n_outer, n_inner = mesh.shape['ep2'], mesh.shape['ep']
    row_spec = P(('dp', 'ep2', 'ep'), None)
    weight_spec = P(('ep2', 'ep'), None, None)
    order = offsets_in_order(n_outer, n_inner)

    def local_step(tokens, expert_idx, gates, w_gate, w_up, w_down):
        rows, d_model = tokens.shape
        top_k = expert_idx.shape[1]
        d_ff = w_gate.shape[2]
        n_dev = n_outer * n_inner
        n_slots = rows * top_k
        any_spec = pl.BlockSpec(memory_space=pl.ANY)
        dma = pltpu.SemaphoreType.DMA
        mixed = pl.pallas_call(
            functools.partial(layer_kernel, order, n_outer, n_inner),
            out_shape=jax.ShapeDtypeStruct((rows, d_model), F32),
            in_specs=[any_spec] * 6,
            out_specs=pl.BlockSpec(memory_space=pltpu.VMEM),
            scratch_shapes=[
                pltpu.VMEM((top_k, rows), I32),
                pltpu.VMEM((top_k, rows), F32),
                pltpu.VMEM((rows, d_model), BF16),
                pltpu.VMEM((d_model, d_ff), BF16),
                pltpu.VMEM((d_model, d_ff), BF16),
                pltpu.VMEM((d_ff, d_model), BF16),
                pltpu.VMEM((n_dev, rows), F32),
                pltpu.VMEM((n_slots, rows), BF16),
                pltpu.VMEM((n_slots, n_slots), BF16),
                pltpu.VMEM((rows, 8), F32),
                pltpu.VMEM((n_slots, d_model), BF16),
                pltpu.VMEM((n_slots, d_model), BF16),
                pltpu.VMEM((n_slots // N_GROUPS, d_ff), BF16),
                pltpu.VMEM((n_slots, d_model), BF16),
                pltpu.VMEM((n_slots, d_model), BF16),
                dma((3,)), dma((3,)),
                dma((n_dev,)), dma((n_dev,)), dma((n_dev,)), dma((n_dev,)),
            ],
            compiler_params=pltpu.CompilerParams(collective_id=0, has_side_effects=True,
                                                 vmem_limit_bytes=40 * 1024 * 1024),
        )(expert_idx.T, gates.T, tokens, w_gate, w_up, w_down)
        return (tokens.astype(F32) + mixed).astype(BF16)

    return jax.shard_map(local_step, mesh=mesh, in_specs=(row_spec, row_spec, row_spec, weight_spec, weight_spec, weight_spec),
                         out_specs=row_spec, check_vma=False)
```

```python
import functools

import jax
import jax.numpy as jnp
from jax import lax
from jax.experimental import pallas as pl
from jax.experimental.pallas import tpu as pltpu
from jax.sharding import PartitionSpec as P

MESH = pl.DeviceIdType.MESH
BF16, F32, I32 = jnp.bfloat16, jnp.float32, jnp.int32
N_GROUPS = 4


def offsets_in_order(n_outer, n_inner):
    chips = n_inner // 2
    all_offsets = [(dy, dx, dc) for dc in (0, 1) for dy in range(n_outer) for dx in range(chips)]

    def hops(o):
        dy, dx, dc = o
        return min(dy, n_outer - dy) + min(dx, chips - dx)

    own = (0, 0, 0)
    far = sorted((o for o in all_offsets if o != own), key=lambda o: -hops(o))
    return [own] + far


def layer_kernel(order, n_outer, n_inner, idx_hbm, gate_hbm, tok_hbm, wg_hbm, wu_hbm, wd_hbm, out_ref,
                 idx_ref, gts_ref, tok_ref, wg_ref, wu_ref, wd_ref, slot_ref, sel_ref, perm_ref, gcol_ref,
                 send_ref, recv_ref, h_ref, y_ref, ret_ref,
                 in_sem, w_sem, out_send, out_recv, back_send, back_recv):
    dp, outer, inner = lax.axis_index('dp'), lax.axis_index('ep2'), lax.axis_index('ep')
    chips = n_inner // 2
    chip, core = inner // 2, inner % 2
    n_dev = n_outer * n_inner
    rows, d_model = tok_ref.shape
    top_k = idx_ref.shape[0]
    cap = (rows * top_k) // n_dev
    d_ff = wg_ref.shape[1]
    n_slots = n_dev * cap
    per_group = n_dev // N_GROUPS
    g_rows = n_slots // N_GROUPS

    def peer(o, sign):
        dy, dx, dc = o
        y = lax.rem(outer + (dy if sign > 0 else n_outer - dy), n_outer)
        x = lax.rem(chip + (dx if sign > 0 else chips - dx), chips)
        c = lax.rem(core + dc, 2)
        return y, x * 2 + c

    barrier = pltpu.get_barrier_semaphore()
    for o in order[1:]:
        y, x = peer(o, 1)
        pl.semaphore_signal(barrier, inc=1, device_id=(dp, y, x), device_id_type=MESH)

    idx_copy = pltpu.make_async_copy(idx_hbm, idx_ref, in_sem.at[0])
    tok_copy = pltpu.make_async_copy(tok_hbm, tok_ref, in_sem.at[1])
    gts_copy = pltpu.make_async_copy(gate_hbm, gts_ref, in_sem.at[2])
    w_copies = [pltpu.make_async_copy(h.at[0], v, w_sem.at[i])
                for i, (h, v) in enumerate(((wg_hbm, wg_ref), (wu_hbm, wu_ref), (wd_hbm, wd_ref)))]
    for copy in (idx_copy, tok_copy, gts_copy):
        copy.start()

    idx_copy.wait()
    expert = lax.broadcasted_iota(I32, (n_dev, rows), 0)
    chosen = jnp.zeros((n_dev, rows), F32)
    for j in range(top_k):
        chosen = chosen + jnp.where(idx_ref[j:j + 1, :] == expert, 1.0, 0.0)
    earlier = lax.broadcasted_iota(I32, (rows, rows), 0) < lax.broadcasted_iota(I32, (rows, rows), 1)
    rank = jnp.dot(chosen.astype(BF16), jnp.where(earlier, 1.0, 0.0).astype(BF16), preferred_element_type=F32)
    slot_ref[...] = jnp.where(chosen > 0.5, rank, -1.0)
    place = lax.broadcasted_iota(I32, (cap, rows), 0).astype(F32)
    for q, o in enumerate(order):
        y, x = peer(o, 1)
        row = slot_ref[pl.ds(y * n_inner + x, 1), :]
        sel_ref[q * cap:(q + 1) * cap, :] = jnp.where(row == place, 1.0, 0.0).astype(BF16)

    def copy_out(q):
        y, x = peer(order[q], 1)
        part = pl.ds(q * cap, cap)
        return pltpu.make_async_remote_copy(send_ref.at[part], recv_ref.at[part], out_send.at[q], out_recv.at[q],
                                            device_id=(dp, y, x), device_id_type=MESH)

    def copy_back(q):
        y, x = peer(order[q], -1)
        part = pl.ds(q * cap, cap)
        return pltpu.make_async_remote_copy(y_ref.at[part], ret_ref.at[part], back_send.at[q], back_recv.at[q],
                                            device_id=(dp, y, x), device_id_type=MESH)

    tok_copy.wait()
    for copy in w_copies:
        copy.start()
    for g in range(N_GROUPS):
        block = sel_ref[g * g_rows:(g + 1) * g_rows, :]
        send_ref[g * g_rows:(g + 1) * g_rows, :] = jnp.dot(block, tok_ref[...], preferred_element_type=F32).astype(BF16)
        if g == 0:
            pl.semaphore_wait(barrier, n_dev - 1)
        for q in range(max(1, g * per_group), (g + 1) * per_group):
            copy_out(q).start()
    recv_ref[0:cap, :] = send_ref[0:cap, :]

    gts_copy.wait()
    gate_cols = jnp.transpose(jnp.concatenate([gts_ref[...], jnp.zeros((8 - top_k, rows), F32)], axis=0))
    for j in range(top_k):
        gcol_ref[j] = jnp.broadcast_to(gate_cols[:, j:j + 1], (rows, 128))
    for g in range(N_GROUPS):
        for j in range(top_k):
            parts = []
            for q in range(g * per_group, (g + 1) * per_group):
                y, x = peer(order[q], 1)
                mine = jnp.where(idx_ref[j:j + 1, :] == y * n_inner + x, 1.0, 0.0)
                parts.append(sel_ref[q * cap:(q + 1) * cap, :].astype(F32) * mine)
            perm_ref[j * rows:(j + 1) * rows, g * g_rows:(g + 1) * g_rows] = jnp.transpose(
                jnp.concatenate(parts, axis=0)).astype(BF16)

    for g in range(N_GROUPS):
        for q in range(g * per_group, (g + 1) * per_group):
            if q:
                copy_out(q).wait_recv()
        part = pl.ds(g * g_rows, g_rows)
        if g == 0:
            w_copies[0].wait()
            w_copies[1].wait()

        def up(n, _):
            cols = pl.ds(pl.multiple_of(n * 896, 128), 896)
            a = jnp.dot(recv_ref[part, :], wg_ref[:, cols], preferred_element_type=F32)
            b = jnp.dot(recv_ref[part, :], wu_ref[:, cols], preferred_element_type=F32)
            h_ref[:, cols] = (jax.nn.silu(a) * b).astype(BF16)
            return 0

        lax.fori_loop(0, d_ff // 896, up, 0)
        if g == 0:
            w_copies[2].wait()

        def down(n, _):
            cols = pl.ds(pl.multiple_of(n * 1024, 256), 1024)
            y_ref[part, cols] = jnp.dot(h_ref[...], wd_ref[:, cols], preferred_element_type=F32).astype(BF16)
            return 0

        lax.fori_loop(0, d_model // 1024, down, 0)
        for q in range(g * per_group, (g + 1) * per_group):
            if q:
                copy_back(q).start()
    ret_ref[0:cap, :] = y_ref[0:cap, :]

    for g in range(N_GROUPS):
        for q in range(g * per_group, (g + 1) * per_group):
            if q:
                copy_back(q).wait_recv()

        def combine(n, _):
            cols = pl.ds(pl.multiple_of(n * 1024, 1024), 1024)
            routed = jnp.dot(perm_ref[:, g * g_rows:(g + 1) * g_rows], ret_ref[g * g_rows:(g + 1) * g_rows, cols],
                             preferred_element_type=F32)
            gate = [jnp.concatenate([gcol_ref[j]] * (1024 // 128), axis=1) for j in range(top_k)]
            total = gate[0] * routed[0:rows]
            for j in range(1, top_k):
                total = total + gate[j] * routed[j * rows:(j + 1) * rows]
            out_ref[:, cols] = total if g == 0 else out_ref[:, cols] + total
            return 0

        lax.fori_loop(0, d_model // 1024, combine, 0)
    for q in range(1, n_dev):
        copy_out(q).wait_send()
        copy_back(q).wait_send()


def solution(mesh):
    n_outer, n_inner = mesh.shape['ep2'], mesh.shape['ep']
    row_spec = P(('dp', 'ep2', 'ep'), None)
    weight_spec = P(('ep2', 'ep'), None, None)
    order = offsets_in_order(n_outer, n_inner)

    def local_step(tokens, expert_idx, gates, w_gate, w_up, w_down):
        rows, d_model = tokens.shape
        top_k = expert_idx.shape[1]
        d_ff = w_gate.shape[2]
        n_dev = n_outer * n_inner
        n_slots = rows * top_k
        any_spec = pl.BlockSpec(memory_space=pl.ANY)
        dma = pltpu.SemaphoreType.DMA
        mixed = pl.pallas_call(
            functools.partial(layer_kernel, order, n_outer, n_inner),
            out_shape=jax.ShapeDtypeStruct((rows, d_model), F32),
            in_specs=[any_spec] * 6,
            out_specs=pl.BlockSpec(memory_space=pltpu.VMEM),
            scratch_shapes=[
                pltpu.VMEM((top_k, rows), I32),
                pltpu.VMEM((top_k, rows), F32),
                pltpu.VMEM((rows, d_model), BF16),
                pltpu.VMEM((d_model, d_ff), BF16),
                pltpu.VMEM((d_model, d_ff), BF16),
                pltpu.VMEM((d_ff, d_model), BF16),
                pltpu.VMEM((n_dev, rows), F32),
                pltpu.VMEM((n_slots, rows), BF16),
                pltpu.VMEM((n_slots, n_slots), BF16),
                pltpu.VMEM((top_k, rows, 128), F32),
                pltpu.VMEM((n_slots, d_model), BF16),
                pltpu.VMEM((n_slots, d_model), BF16),
                pltpu.VMEM((n_slots // N_GROUPS, d_ff), BF16),
                pltpu.VMEM((n_slots, d_model), BF16),
                pltpu.VMEM((n_slots, d_model), BF16),
                dma((3,)), dma((3,)),
                dma((n_dev,)), dma((n_dev,)), dma((n_dev,)), dma((n_dev,)),
            ],
            compiler_params=pltpu.CompilerParams(collective_id=0, has_side_effects=True,
                                                 vmem_limit_bytes=40 * 1024 * 1024),
        )(*[pltpu.with_memory_space_constraint(v, pltpu.HBM)
            for v in (expert_idx.T, gates.T, tokens, w_gate, w_up, w_down)])
        return (tokens.astype(F32) + mixed).astype(BF16)

    return jax.shard_map(local_step, mesh=mesh, in_specs=(row_spec, row_spec, row_spec, weight_spec, weight_spec, weight_spec),
                         out_specs=row_spec, check_vma=False)
```

```python
import functools

import jax
import jax.numpy as jnp
from jax import lax
from jax.experimental import pallas as pl
from jax.experimental.pallas import tpu as pltpu
from jax.sharding import PartitionSpec as P

MESH = pl.DeviceIdType.MESH
BF16, F32, I32 = jnp.bfloat16, jnp.float32, jnp.int32
RING = 4
CLOSE = (0, 1, 3)
GROUPS = []
for _dc in (0, 1):
    GROUPS.append([(dx, dy, _dc) for dy in CLOSE for dx in CLOSE][:8])
    GROUPS.append([(3, 3, _dc)] + [(dx, dy, _dc) for dy in range(RING) for dx in range(RING) if 2 in (dx, dy)])
ORDER = sum(GROUPS, [])
SLOT = {o: q for q, o in enumerate(ORDER)}
FIRST = [sum(len(g) for g in GROUPS[:i]) for i in range(len(GROUPS) + 1)]


def layer_kernel(idx_hbm, gate_hbm, tok_hbm, wg_hbm, wu_hbm, wd_hbm, out_ref,
                 idx_ref, gts_ref, tok_ref, near_ref, wg_ref, wu_ref, wd_ref, tab_ref, perm_ref, gcol_ref,
                 gath_ref, recv_ref, x_ref, h_ref, y_ref, ret_ref,
                 in_sem, w_sem, tab_send, tab_recv, own_send, own_recv, relay_send, relay_recv,
                 out_send, out_recv, back_send, back_recv):
    dp, outer, inner = lax.axis_index('dp'), lax.axis_index('ep2'), lax.axis_index('ep')
    chip, core = inner // 2, inner % 2
    top_k, rows = idx_ref.shape
    n_dev = len(ORDER)
    cap = (rows * top_k) // n_dev
    d_model, d_ff = wg_ref.shape
    half = d_model // 2

    def place(dx, dy, dc, sign=1):
        y = lax.rem(outer + (dy if sign > 0 else RING - dy), RING)
        x = lax.rem(chip + (dx if sign > 0 else RING - dx), RING)
        return y, x * 2 + lax.rem(core + dc, 2)

    def expert(dx, dy, dc):
        y, x = place(dx, dy, dc)
        return y * (2 * RING) + x

    def remote(src, dst, send, recv, where):
        return pltpu.make_async_remote_copy(src, dst, send, recv, device_id=(dp, *where), device_id_type=MESH)

    def along(axis, k):
        return place(k, 0, 0) if axis == 0 else place(0, k, 0)

    barrier = pltpu.get_barrier_semaphore()
    for o in ORDER[1:]:
        pl.semaphore_signal(barrier, inc=1, device_id=(dp, *place(*o)), device_id_type=MESH)

    idx_copy = pltpu.make_async_copy(idx_hbm, idx_ref, in_sem.at[0])
    gts_copy = pltpu.make_async_copy(gate_hbm, gts_ref, in_sem.at[1])
    tok_copies = [pltpu.make_async_copy(tok_hbm.at[:, pl.ds(a * half, half)], tok_ref.at[a], in_sem.at[2 + a])
                  for a in (0, 1)]
    w_copies = [pltpu.make_async_copy(h.at[0], v, w_sem.at[i])
                for i, (h, v) in enumerate(((wg_hbm, wg_ref), (wu_hbm, wu_ref), (wd_hbm, wd_ref)))]
    for copy in (idx_copy, *tok_copies, gts_copy):
        copy.start()

    idx_copy.wait()
    ids = lax.broadcasted_iota(I32, (n_dev, rows), 0)
    chosen = jnp.zeros((n_dev, rows), F32)
    for j in range(top_k):
        chosen = chosen + jnp.where(idx_ref[j:j + 1, :] == ids, 1.0, 0.0)
    earlier = lax.broadcasted_iota(I32, (rows, rows), 0) < lax.broadcasted_iota(I32, (rows, rows), 1)
    rank = jnp.dot(chosen.astype(BF16), jnp.where(earlier, 1.0, 0.0).astype(BF16), preferred_element_type=F32)
    table = jnp.where(chosen > 0.5, rank, -1.0)
    tab_ref[0, 0] = table
    tab_ref[1, 0] = table

    started = []

    def go(copies):
        for copy in copies:
            copy.start()
            started.append(copy)

    def own(a, k):
        return remote(tok_ref.at[a], near_ref.at[a, k - 1], own_send.at[a, k // 2], own_recv.at[a, k // 2], along(a, k))

    def relay(a, k):
        part = pl.ds((k // 2) * (rows // 2), rows // 2)
        return remote(near_ref.at[a, k - 1, part], near_ref.at[a, 1, part],
                      relay_send.at[a, k // 2], relay_recv.at[a, k // 2], along(a, k))

    def table_to(a, k):
        return remote(tab_ref.at[a, 0], tab_ref.at[a, k], tab_send.at[a, k - 1], tab_recv.at[a, k - 1], along(a, k))

    def block(a, i, d, dc):
        q = SLOT[(i, d, dc) if a == 0 else (d, i, dc)]
        return remote(gath_ref.at[a, i, pl.ds((dc * RING + d) * cap, cap)], recv_ref.at[a, pl.ds(q * cap, cap)],
                      out_send.at[a, q], out_recv.at[a, q], place(0, d, dc) if a == 0 else place(d, 0, dc))

    def blocks(i, dc):
        return [block(a, i, d, dc) for d in (2, 1, 3, 0) for a in (0, 1) if d or dc]

    rank_of = lax.broadcasted_iota(I32, (cap, rows), 0).astype(F32)

    def picks(a, i, e):
        return jnp.where(tab_ref[a, i, pl.ds(e, 1), :] == rank_of, 1.0, 0.0).astype(BF16)

    def gather(a, i):
        picked = jnp.concatenate(
            [picks(a, i, expert(0, d, dc) if a == 0 else expert(d, 0, dc)) for dc in (0, 1) for d in range(RING)], axis=0)
        source = tok_ref[a] if i == 0 else near_ref[a, i - 1]
        gath_ref[a, i] = jnp.dot(picked, source, preferred_element_type=F32).astype(BF16)

    for copy in tok_copies:
        copy.wait()
    pl.semaphore_wait(barrier, n_dev - 1)
    go([own(a, k) for a in (0, 1) for k in (1, 3)])
    go([table_to(a, k) for k in (2, 1, 3) for a in (0, 1)])
    for copy in w_copies:
        copy.start()
    gather(0, 0)
    gather(1, 0)
    go(blocks(0, 0))
    for k in (1, 3):
        for a in (0, 1):
            own(a, k).wait_recv()
            go([relay(a, k)])
    for k in (1, 3, 2):
        for a in (0, 1):
            table_to(a, k).wait_recv()
    for k in (1, 3):
        for a in (0, 1):
            gather(a, k)
        go(blocks(k, 0))
    go(blocks(0, 1))
    for k in (1, 3):
        for a in (0, 1):
            relay(a, k).wait_recv()
    for a in (0, 1):
        gather(a, 2)
    go(blocks(2, 0) + blocks(1, 1) + blocks(3, 1) + blocks(2, 1))
    for i in range(RING):
        for a in (0, 1):
            q = SLOT[(i, 0, 0) if a == 0 else (0, i, 0)]
            recv_ref[a, q * cap:(q + 1) * cap, :] = gath_ref[a, i, 0:cap, :]

    gts_copy.wait()
    gate_cols = jnp.transpose(jnp.concatenate([gts_ref[...], jnp.zeros((8 - top_k, rows), F32)], axis=0))
    for j in range(top_k):
        gcol_ref[j] = jnp.broadcast_to(gate_cols[:, j:j + 1], (rows, 128))
    per = 128 // cap
    for g in range(n_dev // per):
        for j in range(top_k):
            parts = []
            for q in range(g * per, (g + 1) * per):
                e = expert(*ORDER[q])
                mine = jnp.where(idx_ref[j:j + 1, :] == e, 1.0, 0.0)
                parts.append(jnp.where(tab_ref[0, 0, pl.ds(e, 1), :] == rank_of, 1.0, 0.0) * mine)
            perm_ref[j * rows:(j + 1) * rows, g * 128:(g + 1) * 128] = jnp.transpose(
                jnp.concatenate(parts, axis=0)).astype(BF16)

    def back(o):
        part = pl.ds(SLOT[o] * cap, cap)
        return remote(y_ref.at[part], ret_ref.at[part], back_send.at[SLOT[o]], back_recv.at[SLOT[o]], place(*o, -1))

    def hops(o):
        return sum(min(d, RING - d) for d in o[:2])

    for g, group in enumerate(GROUPS):
        for dx, dy, dc in group:
            if dy or dc:
                block(0, dx, dy, dc).wait_recv()
            if dx or dc:
                block(1, dy, dx, dc).wait_recv()
        n = len(group) * cap
        part = pl.ds(FIRST[g] * cap, n)
        x_ref[0:n, 0:half] = recv_ref[0, part, :]
        x_ref[0:n, half:] = recv_ref[1, part, :]
        if g == 0:
            w_copies[0].wait()
            w_copies[1].wait()

        def up(m, _):
            cols = pl.ds(pl.multiple_of(m * (d_ff // 2), 128), d_ff // 2)
            a = jnp.dot(x_ref[0:n, :], wg_ref[:, cols], preferred_element_type=F32)
            b = jnp.dot(x_ref[0:n, :], wu_ref[:, cols], preferred_element_type=F32)
            h_ref[0:n, cols] = (jax.nn.silu(a) * b).astype(BF16)
            return 0

        lax.fori_loop(0, 2, up, 0)
        if g == 0:
            w_copies[2].wait()

        def down(m, _):
            cols = pl.ds(pl.multiple_of(m * half, half), half)
            y_ref[part, cols] = jnp.dot(h_ref[0:n, :], wd_ref[:, cols], preferred_element_type=F32).astype(BF16)
            return 0

        lax.fori_loop(0, 2, down, 0)
        for o in group:
            if any(o):
                copy = back(o)
                copy.start()
                started.append(copy)
    own_part = pl.ds(0, cap)
    ret_ref[own_part, :] = y_ref[own_part, :]

    span = n_dev * cap // 2
    for g in (0, 1):
        for o in GROUPS[2 * g] + GROUPS[2 * g + 1]:
            if any(o):
                back(o).wait_recv()
        part = pl.ds(g * span, span)

        def combine(m, _):
            cols = pl.ds(pl.multiple_of(m * half, half), half)
            routed = jnp.dot(perm_ref[:, g * span:(g + 1) * span], ret_ref[part, cols], preferred_element_type=F32)
            total = None
            for j in range(top_k):
                gate = jnp.concatenate([gcol_ref[j]] * (half // 128), axis=1)
                term = gate * routed[j * rows:(j + 1) * rows]
                total = term if j == 0 else total + term
            out_ref[:, cols] = total if g == 0 else out_ref[:, cols] + total
            return 0

        lax.fori_loop(0, 2, combine, 0)
    for copy in started:
        copy.wait_send()


def solution(mesh):
    assert mesh.shape['ep2'] == RING and mesh.shape['ep'] == 2 * RING
    row_spec = P(('dp', 'ep2', 'ep'), None)
    weight_spec = P(('ep2', 'ep'), None, None)

    def local_step(tokens, expert_idx, gates, w_gate, w_up, w_down):
        rows, d_model = tokens.shape
        top_k = expert_idx.shape[1]
        d_ff = w_gate.shape[2]
        n_dev = len(ORDER)
        n_slots = rows * top_k
        cap = n_slots // n_dev
        half = d_model // 2
        most = max(len(g) for g in GROUPS) * cap
        dma = pltpu.SemaphoreType.DMA
        mixed = pl.pallas_call(
            layer_kernel,
            out_shape=jax.ShapeDtypeStruct((rows, d_model), F32),
            in_specs=[pl.BlockSpec(memory_space=pl.ANY)] * 6,
            out_specs=pl.BlockSpec(memory_space=pltpu.VMEM),
            scratch_shapes=[
                pltpu.VMEM((top_k, rows), I32),
                pltpu.VMEM((top_k, rows), F32),
                pltpu.VMEM((2, rows, half), BF16),
                pltpu.VMEM((2, RING - 1, rows, half), BF16),
                pltpu.VMEM((d_model, d_ff), BF16),
                pltpu.VMEM((d_model, d_ff), BF16),
                pltpu.VMEM((d_ff, d_model), BF16),
                pltpu.VMEM((2, RING, n_dev, rows), F32),
                pltpu.VMEM((n_slots, n_slots), BF16),
                pltpu.VMEM((top_k, rows, 128), F32),
                pltpu.VMEM((2, RING, 2 * RING * cap, half), BF16),
                pltpu.VMEM((2, n_slots, half), BF16),
                pltpu.VMEM((most, d_model), BF16),
                pltpu.VMEM((most, d_ff), BF16),
                pltpu.VMEM((n_slots, d_model), BF16),
                pltpu.VMEM((n_slots, d_model), BF16),
                dma((4,)), dma((3,)), dma((2, 3)), dma((2, 3)), dma((2, 2)), dma((2, 2)), dma((2, 2)), dma((2, 2)),
                dma((2, n_dev)), dma((2, n_dev)), dma((n_dev,)), dma((n_dev,)),
            ],
            compiler_params=pltpu.CompilerParams(collective_id=0, has_side_effects=True,
                                                 vmem_limit_bytes=44 * 1024 * 1024),
        )(*[pltpu.with_memory_space_constraint(v, pltpu.HBM)
            for v in (expert_idx.T, gates.T, tokens, w_gate, w_up, w_down)])
        return (tokens.astype(F32) + mixed).astype(BF16)

    return jax.shard_map(local_step, mesh=mesh, in_specs=(row_spec, row_spec, row_spec, weight_spec, weight_spec, weight_spec),
                         out_specs=row_spec, check_vma=False)
```

```python
import functools

import jax
import jax.numpy as jnp
from jax import lax
from jax.experimental import pallas as pl
from jax.experimental.pallas import tpu as pltpu
from jax.sharding import PartitionSpec as P

MESH = pl.DeviceIdType.MESH
BF16, F32, I32 = jnp.bfloat16, jnp.float32, jnp.int32
RING = 4
CLOSE = (0, 1, 3)
GROUPS = []
for _dc in (0, 1):
    GROUPS.append([(dx, dy, _dc) for dy in CLOSE for dx in CLOSE][:8])
    GROUPS.append([(3, 3, _dc)] + [(dx, dy, _dc) for dy in range(RING) for dx in range(RING) if 2 in (dx, dy)])
ORDER = sum(GROUPS, [])
SLOT = {o: q for q, o in enumerate(ORDER)}
FIRST = [sum(len(g) for g in GROUPS[:i]) for i in range(len(GROUPS) + 1)]


def layer_kernel(idx_hbm, gate_hbm, tok_hbm, wg_hbm, wu_hbm, wd_hbm, out_ref,
                 idx_ref, gts_ref, tok_ref, near_ref, wg_ref, wu_ref, wd_ref, tab_ref, perm_ref, gcol_ref,
                 gath_ref, recv_ref, x_ref, h_ref, y_ref, ret_ref,
                 in_sem, w_sem, tab_send, tab_recv, own_send, own_recv, relay_send, relay_recv,
                 out_send, out_recv, back_send, back_recv):
    dp, outer, inner = lax.axis_index('dp'), lax.axis_index('ep2'), lax.axis_index('ep')
    chip, core = inner // 2, inner % 2
    top_k, rows = idx_ref.shape
    n_dev = len(ORDER)
    cap = (rows * top_k) // n_dev
    d_model, d_ff = wg_ref.shape
    half = d_model // 2

    def place(dx, dy, dc, sign=1):
        y = lax.rem(outer + (dy if sign > 0 else RING - dy), RING)
        x = lax.rem(chip + (dx if sign > 0 else RING - dx), RING)
        return y, x * 2 + lax.rem(core + dc, 2)

    def expert(dx, dy, dc):
        y, x = place(dx, dy, dc)
        return y * (2 * RING) + x

    def remote(src, dst, send, recv, where):
        return pltpu.make_async_remote_copy(src, dst, send, recv, device_id=(dp, *where), device_id_type=MESH)

    def along(axis, k):
        return place(k, 0, 0) if axis == 0 else place(0, k, 0)

    barrier = pltpu.get_barrier_semaphore()
    for o in ORDER[1:]:
        pl.semaphore_signal(barrier, inc=1, device_id=(dp, *place(*o)), device_id_type=MESH)

    idx_copy = pltpu.make_async_copy(idx_hbm, idx_ref, in_sem.at[0])
    gts_copy = pltpu.make_async_copy(gate_hbm, gts_ref, in_sem.at[1])
    tok_copies = [pltpu.make_async_copy(tok_hbm.at[:, pl.ds(a * half, half)], tok_ref.at[a], in_sem.at[2 + a])
                  for a in (0, 1)]
    w_copies = [pltpu.make_async_copy(h.at[0], v, w_sem.at[i])
                for i, (h, v) in enumerate(((wg_hbm, wg_ref), (wu_hbm, wu_ref), (wd_hbm, wd_ref)))]
    for copy in (idx_copy, *tok_copies, gts_copy):
        copy.start()

    idx_copy.wait()
    ids = lax.broadcasted_iota(I32, (n_dev, rows), 0)
    chosen = jnp.zeros((n_dev, rows), F32)
    for j in range(top_k):
        chosen = chosen + jnp.where(idx_ref[j:j + 1, :] == ids, 1.0, 0.0)
    earlier = lax.broadcasted_iota(I32, (rows, rows), 0) < lax.broadcasted_iota(I32, (rows, rows), 1)
    rank = jnp.dot(chosen.astype(BF16), jnp.where(earlier, 1.0, 0.0).astype(BF16), preferred_element_type=F32)
    table = jnp.where(chosen > 0.5, rank, -1.0)
    tab_ref[0, 0] = table
    tab_ref[1, 0] = table

    started = []

    def go(copies):
        for copy in copies:
            copy.start()
            started.append(copy)

    def own(a, k):
        return remote(tok_ref.at[a], near_ref.at[a, k - 1], own_send.at[a, k // 2], own_recv.at[a, k // 2], along(a, k))

    def relay(a, k):
        part = pl.ds((k // 2) * (rows // 2), rows // 2)
        return remote(near_ref.at[a, k - 1, part], near_ref.at[a, 1, part],
                      relay_send.at[a, k // 2], relay_recv.at[a, k // 2], along(a, k))

    def table_to(a, k):
        return remote(tab_ref.at[a, 0], tab_ref.at[a, k], tab_send.at[a, k - 1], tab_recv.at[a, k - 1], along(a, k))

    def block(a, i, d, dc):
        q = SLOT[(i, d, dc) if a == 0 else (d, i, dc)]
        return remote(gath_ref.at[a, i, pl.ds((dc * RING + d) * cap, cap)], recv_ref.at[a, pl.ds(q * cap, cap)],
                      out_send.at[a, q], out_recv.at[a, q], place(0, d, dc) if a == 0 else place(d, 0, dc))

    def blocks(i, dc):
        return [block(a, i, d, dc) for d in (0, 1, 3, 2) for a in (0, 1) if d or dc]

    rank_of = lax.broadcasted_iota(I32, (cap, rows), 0).astype(F32)

    def picks(a, i, e):
        return jnp.where(tab_ref[a, i, pl.ds(e, 1), :] == rank_of, 1.0, 0.0).astype(BF16)

    def gather(a, i):
        picked = jnp.concatenate(
            [picks(a, i, expert(0, d, dc) if a == 0 else expert(d, 0, dc)) for dc in (0, 1) for d in range(RING)], axis=0)
        source = tok_ref[a] if i == 0 else near_ref[a, i - 1]
        gath_ref[a, i] = jnp.dot(picked, source, preferred_element_type=F32).astype(BF16)

    for copy in tok_copies:
        copy.wait()
    pl.semaphore_wait(barrier, n_dev - 1)
    go([own(a, k) for a in (0, 1) for k in (1, 3)])
    go([table_to(a, k) for k in (2, 1, 3) for a in (0, 1)])
    for copy in w_copies:
        copy.start()
    gather(0, 0)
    gather(1, 0)
    go(blocks(0, 0))
    for k in (1, 3):
        for a in (0, 1):
            own(a, k).wait_recv()
            go([relay(a, k)])
    for k in (1, 3, 2):
        for a in (0, 1):
            table_to(a, k).wait_recv()
    for k in (1, 3):
        for a in (0, 1):
            gather(a, k)
        go(blocks(k, 0))
    go(blocks(0, 1))
    for k in (1, 3):
        for a in (0, 1):
            relay(a, k).wait_recv()
    for a in (0, 1):
        gather(a, 2)
    go(blocks(2, 0) + blocks(1, 1) + blocks(3, 1) + blocks(2, 1))
    for i in range(RING):
        for a in (0, 1):
            q = SLOT[(i, 0, 0) if a == 0 else (0, i, 0)]
            recv_ref[a, q * cap:(q + 1) * cap, :] = gath_ref[a, i, 0:cap, :]

    gts_copy.wait()
    gate_cols = jnp.transpose(jnp.concatenate([gts_ref[...], jnp.zeros((8 - top_k, rows), F32)], axis=0))
    for j in range(top_k):
        gcol_ref[j] = jnp.broadcast_to(gate_cols[:, j:j + 1], (rows, 128))
    per = 128 // cap
    for g in range(n_dev // per):
        for j in range(top_k):
            parts = []
            for q in range(g * per, (g + 1) * per):
                e = expert(*ORDER[q])
                mine = jnp.where(idx_ref[j:j + 1, :] == e, 1.0, 0.0)
                parts.append(jnp.where(tab_ref[0, 0, pl.ds(e, 1), :] == rank_of, 1.0, 0.0) * mine)
            perm_ref[j * rows:(j + 1) * rows, g * 128:(g + 1) * 128] = jnp.transpose(
                jnp.concatenate(parts, axis=0)).astype(BF16)

    def back(o):
        part = pl.ds(SLOT[o] * cap, cap)
        return remote(y_ref.at[part], ret_ref.at[part], back_send.at[SLOT[o]], back_recv.at[SLOT[o]], place(*o, -1))

    def hops(o):
        return sum(min(d, RING - d) for d in o[:2])

    for g, group in enumerate(GROUPS):
        for dx, dy, dc in group:
            if dy or dc:
                block(0, dx, dy, dc).wait_recv()
            if dx or dc:
                block(1, dy, dx, dc).wait_recv()
        n = len(group) * cap
        part = pl.ds(FIRST[g] * cap, n)
        x_ref[0:n, 0:half] = recv_ref[0, part, :]
        x_ref[0:n, half:] = recv_ref[1, part, :]
        if g == 0:
            w_copies[0].wait()
            w_copies[1].wait()

        def up(m, _):
            cols = pl.ds(pl.multiple_of(m * (d_ff // 2), 128), d_ff // 2)
            a = jnp.dot(x_ref[0:n, :], wg_ref[:, cols], preferred_element_type=F32)
            b = jnp.dot(x_ref[0:n, :], wu_ref[:, cols], preferred_element_type=F32)
            h_ref[0:n, cols] = (jax.nn.silu(a) * b).astype(BF16)
            return 0

        lax.fori_loop(0, 2, up, 0)
        if g == 0:
            w_copies[2].wait()

        def down(m, _):
            cols = pl.ds(pl.multiple_of(m * half, half), half)
            y_ref[part, cols] = jnp.dot(h_ref[0:n, :], wd_ref[:, cols], preferred_element_type=F32).astype(BF16)
            return 0

        lax.fori_loop(0, 2, down, 0)
        for o in sorted(group, key=lambda o: -hops(o)) if g == 3 else group:
            if any(o):
                copy = back(o)
                copy.start()
                started.append(copy)
    early = len(started) - len(GROUPS[-1]) - len(GROUPS[-2])
    for copy in started[:early]:
        copy.wait_send()
    own_part = pl.ds(0, cap)
    ret_ref[own_part, :] = y_ref[own_part, :]

    span = n_dev * cap // 2
    for g in (0, 1):
        for o in GROUPS[2 * g] + GROUPS[2 * g + 1]:
            if any(o):
                back(o).wait_recv()
        part = pl.ds(g * span, span)

        def combine(m, _):
            cols = pl.ds(pl.multiple_of(m * half, half), half)
            routed = jnp.dot(perm_ref[:, g * span:(g + 1) * span], ret_ref[part, cols], preferred_element_type=F32)
            total = None
            for j in range(top_k):
                gate = jnp.concatenate([gcol_ref[j]] * (half // 128), axis=1)
                term = gate * routed[j * rows:(j + 1) * rows]
                total = term if j == 0 else total + term
            out_ref[:, cols] = total if g == 0 else out_ref[:, cols] + total
            return 0

        lax.fori_loop(0, 2, combine, 0)
    for copy in started[early:]:
        copy.wait_send()


def solution(mesh):
    assert mesh.shape['ep2'] == RING and mesh.shape['ep'] == 2 * RING
    row_spec = P(('dp', 'ep2', 'ep'), None)
    weight_spec = P(('ep2', 'ep'), None, None)

    def local_step(tokens, expert_idx, gates, w_gate, w_up, w_down):
        rows, d_model = tokens.shape
        top_k = expert_idx.shape[1]
        d_ff = w_gate.shape[2]
        n_dev = len(ORDER)
        n_slots = rows * top_k
        cap = n_slots // n_dev
        half = d_model // 2
        most = max(len(g) for g in GROUPS) * cap
        dma = pltpu.SemaphoreType.DMA
        mixed = pl.pallas_call(
            layer_kernel,
            out_shape=jax.ShapeDtypeStruct((rows, d_model), F32),
            in_specs=[pl.BlockSpec(memory_space=pl.ANY)] * 6,
            out_specs=pl.BlockSpec(memory_space=pltpu.VMEM),
            scratch_shapes=[
                pltpu.VMEM((top_k, rows), I32),
                pltpu.VMEM((top_k, rows), F32),
                pltpu.VMEM((2, rows, half), BF16),
                pltpu.VMEM((2, RING - 1, rows, half), BF16),
                pltpu.VMEM((d_model, d_ff), BF16),
                pltpu.VMEM((d_model, d_ff), BF16),
                pltpu.VMEM((d_ff, d_model), BF16),
                pltpu.VMEM((2, RING, n_dev, rows), F32),
                pltpu.VMEM((n_slots, n_slots), BF16),
                pltpu.VMEM((top_k, rows, 128), F32),
                pltpu.VMEM((2, RING, 2 * RING * cap, half), BF16),
                pltpu.VMEM((2, n_slots, half), BF16),
                pltpu.VMEM((most, d_model), BF16),
                pltpu.VMEM((most, d_ff), BF16),
                pltpu.VMEM((n_slots, d_model), BF16),
                pltpu.VMEM((n_slots, d_model), BF16),
                dma((4,)), dma((3,)), dma((2, 3)), dma((2, 3)), dma((2, 2)), dma((2, 2)), dma((2, 2)), dma((2, 2)),
                dma((2, n_dev)), dma((2, n_dev)), dma((n_dev,)), dma((n_dev,)),
            ],
            compiler_params=pltpu.CompilerParams(collective_id=0, has_side_effects=True,
                                                 vmem_limit_bytes=44 * 1024 * 1024),
        )(*[pltpu.with_memory_space_constraint(v, pltpu.HBM)
            for v in (expert_idx.T, gates.T, tokens, w_gate, w_up, w_down)])
        return (tokens.astype(F32) + mixed).astype(BF16)

    return jax.shard_map(local_step, mesh=mesh, in_specs=(row_spec, row_spec, row_spec, weight_spec, weight_spec, weight_spec),
                         out_specs=row_spec, check_vma=False)
```

```python
import functools

import jax
import jax.numpy as jnp
from jax import lax
from jax.experimental import pallas as pl
from jax.experimental.pallas import tpu as pltpu
from jax.sharding import PartitionSpec as P

MESH = pl.DeviceIdType.MESH
BF16, F32, I32 = jnp.bfloat16, jnp.float32, jnp.int32
RING = 4
CLOSE = (0, 1, 3)
GROUPS = []
for _dc in (0, 1):
    GROUPS.append([(dx, dy, _dc) for dy in CLOSE for dx in CLOSE][:8])
    GROUPS.append([(3, 3, _dc)] + [(dx, dy, _dc) for dy in range(RING) for dx in range(RING) if 2 in (dx, dy)])
ORDER = sum(GROUPS, [])
SLOT = {o: q for q, o in enumerate(ORDER)}
FIRST = [sum(len(g) for g in GROUPS[:i]) for i in range(len(GROUPS) + 1)]


def layer_kernel(idx_hbm, gate_hbm, tok_hbm, wg_hbm, wu_hbm, wd_hbm, out_ref,
                 idx_ref, gts_ref, tok_ref, near_ref, wg_ref, wu_ref, wd_ref, tab_ref, perm_ref, gcol_ref,
                 gath_ref, recv_ref, x_ref, h_ref, y_ref, ret_ref,
                 in_sem, w_sem, tab_send, tab_recv, own_send, own_recv, relay_send, relay_recv,
                 out_send, out_recv, back_send, back_recv):
    dp, outer, inner = lax.axis_index('dp'), lax.axis_index('ep2'), lax.axis_index('ep')
    chip, core = inner // 2, inner % 2
    top_k, rows = idx_ref.shape
    n_dev = len(ORDER)
    cap = (rows * top_k) // n_dev
    d_model, d_ff = wg_ref.shape
    half = d_model // 2

    def place(dx, dy, dc, sign=1):
        y = lax.rem(outer + (dy if sign > 0 else RING - dy), RING)
        x = lax.rem(chip + (dx if sign > 0 else RING - dx), RING)
        return y, x * 2 + lax.rem(core + dc, 2)

    def expert(dx, dy, dc):
        y, x = place(dx, dy, dc)
        return y * (2 * RING) + x

    def remote(src, dst, send, recv, where):
        return pltpu.make_async_remote_copy(src, dst, send, recv, device_id=(dp, *where), device_id_type=MESH)

    def along(axis, k):
        return place(k, 0, 0) if axis == 0 else place(0, k, 0)

    barrier = pltpu.get_barrier_semaphore()
    for o in ORDER[1:]:
        pl.semaphore_signal(barrier, inc=1, device_id=(dp, *place(*o)), device_id_type=MESH)

    idx_copy = pltpu.make_async_copy(idx_hbm, idx_ref, in_sem.at[0])
    gts_copy = pltpu.make_async_copy(gate_hbm, gts_ref, in_sem.at[1])
    tok_copies = [pltpu.make_async_copy(tok_hbm.at[:, pl.ds(a * half, half)], tok_ref.at[a], in_sem.at[2 + a])
                  for a in (0, 1)]
    w_copies = [pltpu.make_async_copy(h.at[0], v, w_sem.at[i])
                for i, (h, v) in enumerate(((wg_hbm, wg_ref), (wu_hbm, wu_ref), (wd_hbm, wd_ref)))]
    for copy in (*tok_copies, idx_copy, gts_copy):
        copy.start()

    started = []

    def go(copies):
        for copy in copies:
            copy.start()
            started.append(copy)

    def own(a, k):
        return remote(tok_ref.at[a], near_ref.at[a, k - 1], own_send.at[a, k // 2], own_recv.at[a, k // 2], along(a, k))

    def relay(a, k):
        part = pl.ds((k // 2) * (rows // 2), rows // 2)
        return remote(near_ref.at[a, k - 1, part], near_ref.at[a, 1, part],
                      relay_send.at[a, k // 2], relay_recv.at[a, k // 2], along(a, k))

    def table_to(a, k):
        return remote(tab_ref.at[a, 0], tab_ref.at[a, k], tab_send.at[a, k - 1], tab_recv.at[a, k - 1], along(a, k))

    def block(a, i, d, dc):
        q = SLOT[(i, d, dc) if a == 0 else (d, i, dc)]
        return remote(gath_ref.at[a, i, pl.ds((dc * RING + d) * cap, cap)], recv_ref.at[a, pl.ds(q * cap, cap)],
                      out_send.at[a, q], out_recv.at[a, q], place(0, d, dc) if a == 0 else place(d, 0, dc))

    def blocks(i, dc):
        return [block(a, i, d, dc) for d in (0, 1, 3, 2) for a in (0, 1) if d or dc]

    rank_of = lax.broadcasted_iota(I32, (cap, rows), 0).astype(F32)

    def picks(a, i, e):
        return jnp.where(tab_ref[a, i, pl.ds(e, 1), :] == rank_of, 1.0, 0.0).astype(BF16)

    def gather(a, i):
        picked = jnp.concatenate(
            [picks(a, i, expert(0, d, dc) if a == 0 else expert(d, 0, dc)) for dc in (0, 1) for d in range(RING)], axis=0)
        source = tok_ref[a] if i == 0 else near_ref[a, i - 1]
        gath_ref[a, i] = jnp.dot(picked, source, preferred_element_type=F32).astype(BF16)

    for copy in tok_copies:
        copy.wait()
    pl.semaphore_wait(barrier, n_dev - 1)
    go([own(a, k) for a in (0, 1) for k in (1, 3)])

    idx_copy.wait()
    ids = lax.broadcasted_iota(I32, (n_dev, rows), 0)
    chosen = jnp.zeros((n_dev, rows), F32)
    for j in range(top_k):
        chosen = chosen + jnp.where(idx_ref[j:j + 1, :] == ids, 1.0, 0.0)
    earlier = lax.broadcasted_iota(I32, (rows, rows), 0) < lax.broadcasted_iota(I32, (rows, rows), 1)
    rank = jnp.dot(chosen.astype(BF16), jnp.where(earlier, 1.0, 0.0).astype(BF16), preferred_element_type=F32)
    table = jnp.where(chosen > 0.5, rank, -1.0)
    tab_ref[0, 0] = table
    tab_ref[1, 0] = table

    go([table_to(a, k) for k in (2, 1, 3) for a in (0, 1)])
    for copy in w_copies:
        copy.start()
    gather(0, 0)
    gather(1, 0)
    go(blocks(0, 0))
    for k in (1, 3):
        for a in (0, 1):
            own(a, k).wait_recv()
            go([relay(a, k)])
    for k in (1, 3, 2):
        for a in (0, 1):
            table_to(a, k).wait_recv()
    for k in (1, 3):
        for a in (0, 1):
            gather(a, k)
        go(blocks(k, 0))
    go(blocks(0, 1))
    for k in (1, 3):
        for a in (0, 1):
            relay(a, k).wait_recv()
    for a in (0, 1):
        gather(a, 2)
    go(blocks(2, 0) + blocks(1, 1) + blocks(3, 1) + blocks(2, 1))
    for i in range(RING):
        for a in (0, 1):
            q = SLOT[(i, 0, 0) if a == 0 else (0, i, 0)]
            recv_ref[a, q * cap:(q + 1) * cap, :] = gath_ref[a, i, 0:cap, :]

    gts_copy.wait()
    gate_cols = jnp.transpose(jnp.concatenate([gts_ref[...], jnp.zeros((8 - top_k, rows), F32)], axis=0))
    for j in range(top_k):
        gcol_ref[j] = jnp.broadcast_to(gate_cols[:, j:j + 1], (rows, 128))
    per = 128 // cap
    for g in range(n_dev // per):
        for j in range(top_k):
            parts = []
            for q in range(g * per, (g + 1) * per):
                e = expert(*ORDER[q])
                mine = jnp.where(idx_ref[j:j + 1, :] == e, 1.0, 0.0)
                parts.append(jnp.where(tab_ref[0, 0, pl.ds(e, 1), :] == rank_of, 1.0, 0.0) * mine)
            perm_ref[j * rows:(j + 1) * rows, g * 128:(g + 1) * 128] = jnp.transpose(
                jnp.concatenate(parts, axis=0)).astype(BF16)

    def back(o):
        part = pl.ds(SLOT[o] * cap, cap)
        return remote(y_ref.at[part], ret_ref.at[part], back_send.at[SLOT[o]], back_recv.at[SLOT[o]], place(*o, -1))

    def hops(o):
        return sum(min(d, RING - d) for d in o[:2])

    for g, group in enumerate(GROUPS):
        for dx, dy, dc in group:
            if dy or dc:
                block(0, dx, dy, dc).wait_recv()
            if dx or dc:
                block(1, dy, dx, dc).wait_recv()
        n = len(group) * cap
        part = pl.ds(FIRST[g] * cap, n)
        x_ref[0:n, 0:half] = recv_ref[0, part, :]
        x_ref[0:n, half:] = recv_ref[1, part, :]
        if g == 0:
            w_copies[0].wait()
            w_copies[1].wait()

        def up(m, _):
            cols = pl.ds(pl.multiple_of(m * (d_ff // 2), 128), d_ff // 2)
            a = jnp.dot(x_ref[0:n, :], wg_ref[:, cols], preferred_element_type=F32)
            b = jnp.dot(x_ref[0:n, :], wu_ref[:, cols], preferred_element_type=F32)
            h_ref[0:n, cols] = (jax.nn.silu(a) * b).astype(BF16)
            return 0

        lax.fori_loop(0, 2, up, 0)
        if g == 0:
            w_copies[2].wait()

        def down(m, _):
            cols = pl.ds(pl.multiple_of(m * half, half), half)
            y_ref[part, cols] = jnp.dot(h_ref[0:n, :], wd_ref[:, cols], preferred_element_type=F32).astype(BF16)
            return 0

        lax.fori_loop(0, 2, down, 0)
        for o in sorted(group, key=lambda o: -hops(o)) if g == 3 else group:
            if any(o):
                copy = back(o)
                copy.start()
                started.append(copy)
    early = len(started) - len(GROUPS[-1]) - len(GROUPS[-2])
    for copy in started[:early]:
        copy.wait_send()
    own_part = pl.ds(0, cap)
    ret_ref[own_part, :] = y_ref[own_part, :]

    span = n_dev * cap // 2
    for g in (0, 1):
        for o in GROUPS[2 * g] + GROUPS[2 * g + 1]:
            if any(o):
                back(o).wait_recv()
        part = pl.ds(g * span, span)

        def combine(m, _):
            cols = pl.ds(pl.multiple_of(m * half, half), half)
            routed = jnp.dot(perm_ref[:, g * span:(g + 1) * span], ret_ref[part, cols], preferred_element_type=F32)
            total = None
            for j in range(top_k):
                gate = jnp.concatenate([gcol_ref[j]] * (half // 128), axis=1)
                term = gate * routed[j * rows:(j + 1) * rows]
                total = term if j == 0 else total + term
            out_ref[:, cols] = total if g == 0 else out_ref[:, cols] + total
            return 0

        lax.fori_loop(0, 2, combine, 0)
    for copy in started[early:]:
        copy.wait_send()


def solution(mesh):
    assert mesh.shape['ep2'] == RING and mesh.shape['ep'] == 2 * RING
    row_spec = P(('dp', 'ep2', 'ep'), None)
    weight_spec = P(('ep2', 'ep'), None, None)

    def local_step(tokens, expert_idx, gates, w_gate, w_up, w_down):
        rows, d_model = tokens.shape
        top_k = expert_idx.shape[1]
        d_ff = w_gate.shape[2]
        n_dev = len(ORDER)
        n_slots = rows * top_k
        cap = n_slots // n_dev
        half = d_model // 2
        most = max(len(g) for g in GROUPS) * cap
        dma = pltpu.SemaphoreType.DMA
        mixed = pl.pallas_call(
            layer_kernel,
            out_shape=jax.ShapeDtypeStruct((rows, d_model), F32),
            in_specs=[pl.BlockSpec(memory_space=pl.ANY)] * 6,
            out_specs=pl.BlockSpec(memory_space=pltpu.VMEM),
            scratch_shapes=[
                pltpu.VMEM((top_k, rows), I32),
                pltpu.VMEM((top_k, rows), F32),
                pltpu.VMEM((2, rows, half), BF16),
                pltpu.VMEM((2, RING - 1, rows, half), BF16),
                pltpu.VMEM((d_model, d_ff), BF16),
                pltpu.VMEM((d_model, d_ff), BF16),
                pltpu.VMEM((d_ff, d_model), BF16),
                pltpu.VMEM((2, RING, n_dev, rows), F32),
                pltpu.VMEM((n_slots, n_slots), BF16),
                pltpu.VMEM((top_k, rows, 128), F32),
                pltpu.VMEM((2, RING, 2 * RING * cap, half), BF16),
                pltpu.VMEM((2, n_slots, half), BF16),
                pltpu.VMEM((most, d_model), BF16),
                pltpu.VMEM((most, d_ff), BF16),
                pltpu.VMEM((n_slots, d_model), BF16),
                pltpu.VMEM((n_slots, d_model), BF16),
                dma((4,)), dma((3,)), dma((2, 3)), dma((2, 3)), dma((2, 2)), dma((2, 2)), dma((2, 2)), dma((2, 2)),
                dma((2, n_dev)), dma((2, n_dev)), dma((n_dev,)), dma((n_dev,)),
            ],
            compiler_params=pltpu.CompilerParams(collective_id=0, has_side_effects=True,
                                                 vmem_limit_bytes=44 * 1024 * 1024),
        )(*[pltpu.with_memory_space_constraint(v, pltpu.HBM)
            for v in (expert_idx.T, gates.T, tokens, w_gate, w_up, w_down)])
        return (tokens.astype(F32) + mixed).astype(BF16)

    return jax.shard_map(local_step, mesh=mesh, in_specs=(row_spec, row_spec, row_spec, weight_spec, weight_spec, weight_spec),
                         out_specs=row_spec, check_vma=False)
```
